256 devices in a mesh: wide: 32 (over y, x, core), narrow: 8 (over z).
Axes of the slice: x: 4, y: 4, z: 8, core: 2. Of those that a mesh axis runs over, the one named last changes fastest.
Arguments:
- schur_matrix: bfloat16 [32, 8, 3, 1024, 1024], P('wide', 'narrow')
- face_inverse: bfloat16 [32, 8, 3, 8, 128, 128], P('wide', 'narrow')
- deluxe: bfloat16 [32, 8, 3, 8, 128, 128], P('wide', 'narrow')
- primal_weight: float32 [32, 8, 3, 8, 128], P('wide', 'narrow'), may hold values from 0.05 to 0.3
- coarse_group: float32 [32, 192, 192], P('wide', 'narrow')
- coarse_map: float32 [32, 192, 8], P('wide', 'narrow'), may hold values from -0.4375 to 0.4375
- coarse_top: float32 [256, 256], P('wide')
- load_vector: bfloat16 [32, 8, 3, 8, 128, 128], P('wide', 'narrow'), may hold values from -6 to 6
- previous: bfloat16 [32, 8, 3, 8, 128, 128], P('wide', 'narrow'), may hold values from -3 to 3
- slot_count: int32 [32, 8], P('wide', 'narrow'), may hold values from 1 to 3, as said below
- partner: int32 [32, 8, 3, 8], P('wide', 'narrow'), may hold values from -1 to 2, as said below
- face_size: int32 [32, 8, 3, 8], P('wide', 'narrow'), may hold values from 0 to 128, as said below
Outputs:
- solution: float32 [32, 8, 3, 8, 128, 128], P('wide', 'narrow')
- residual: float32 [32, 8, 3, 8, 128, 128], P('wide', 'narrow')
The draws below stay inside these ranges and needn't reach their ends.
Inputs may be any that keep to these rules, and one draw needn't show every extreme that they name: Slots of a device below its slot_count hold subdomains; the others are empty. partner names the slot of the subdomain across a face as in the reference program; the relation is symmetric (the partner face names this slot back), and it is -1 on empty slots, on faces whose partner slot is empty, on face 0 at narrow index 0 and on face 1 at the last narrow index. `face_size`: both sides of a face with a partner have the same size; faces of empty slots have size 0, all other faces at least 32.
All inputs are finite; a program needn't handle non-finite values.
Results may differ from the reference program's by a relative error of at most 0.00355.
The reference program's roundings to bfloat16 on the way count: a program that leaves them out, or rounds other values in their place, can miss the bound.
Values may be sent and summed in bfloat16 or wider, within the bound.
A program may use at most 128 MiB of HBM per device.

```python
import math
import jax
import jax.numpy as jnp
from jax import lax

FW = 128
NF = 8
SLOTS = 3
NRHS = 128
NQ = 8
ITERS = 2
NB = 1024
SPACE = 32
SLABS = 8
NCG = 192
NT = 256


def look_up(table_in, slot_map):
    return jnp.take_along_axis(table_in, slot_map, axis=2)


def shift_below(table_in, filler):
    pad_row = jnp.full_like(table_in[:, :1], filler)
    return jnp.concatenate([pad_row, table_in[:, :-1]], axis=1)


def shift_above(table_in, filler):
    pad_row = jnp.full_like(table_in[:, :1], filler)
    return jnp.concatenate([table_in[:, 1:], pad_row], axis=1)


def layout_tables(seed_key):
    base_key = jax.random.fold_in(seed_key, 9173)
    levels = jax.random.randint(jax.random.fold_in(base_key, 1), (SPACE, SLABS), 0, 5)
    middle = max(1, SLOTS - 1)
    live_count = jnp.where(levels < 3, 1, jnp.where(levels == 3, middle, SLOTS)).astype(jnp.int32)
    slot_ids = jnp.arange(SLOTS, dtype=jnp.int32)
    alive_slot = slot_ids[None, None, :] < live_count[:, :, None]
    scores = jax.random.randint(jax.random.fold_in(base_key, 2), (SPACE, SLABS, 4, SLOTS), 0, 1 << 20) * SLOTS + slot_ids
    forward = jnp.argsort(scores, axis=-1).astype(jnp.int32)
    backward = jnp.argsort(forward, axis=-1).astype(jnp.int32)
    raw_sizes = jax.random.randint(jax.random.fold_in(base_key, 3), (SPACE, SLABS, SLOTS, NF), FW // 4, FW + 1).astype(jnp.int32)
    wide_next = forward[:, :, 0]
    wide_prev = jnp.roll(backward[:, :, 0], 1, axis=0)
    slab_next = forward[:, :, 1]
    slab_prev = shift_below(backward[:, :, 1], 0)
    slab_ids = jnp.arange(SLABS)
    has_above = (slab_ids < SLABS - 1)[None, :, None]
    has_below = (slab_ids > 0)[None, :, None]
    alive_right = jnp.roll(alive_slot, -1, axis=0)
    alive_left = jnp.roll(alive_slot, 1, axis=0)
    alive_above = shift_above(alive_slot, False)
    alive_below = shift_below(alive_slot, False)
    slot_maps = [slab_prev, slab_next, wide_prev, wide_next, forward[:, :, 2], backward[:, :, 2], forward[:, :, 3], backward[:, :, 3]]
    present = [has_below & look_up(alive_below, slab_prev), has_above & look_up(alive_above, slab_next), look_up(alive_left, wide_prev), look_up(alive_right, wide_next), look_up(alive_slot, forward[:, :, 2]), look_up(alive_slot, backward[:, :, 2]), look_up(alive_slot, forward[:, :, 3]), look_up(alive_slot, backward[:, :, 3])]
    present = [alive_slot & linked for linked in present]
    partner = jnp.stack([jnp.where(linked, slot_map, -1) for linked, slot_map in zip(present, slot_maps)], axis=-1).astype(jnp.int32)
    odd_sizes = [look_up(shift_below(raw_sizes[..., 1], 0), slab_prev), None, look_up(jnp.roll(raw_sizes[..., 3], 1, axis=0), wide_prev), None, look_up(raw_sizes[..., 5], forward[:, :, 2]), None, look_up(raw_sizes[..., 7], forward[:, :, 3]), None]
    size_list = []
    for face_id in range(8):
        own_size = raw_sizes[..., face_id]
        if face_id % 2 == 0:
            own_size = jnp.where(present[face_id], odd_sizes[face_id], own_size)
        size_list.append(own_size)
    face_size = jnp.where(alive_slot[..., None], jnp.stack(size_list, axis=-1), 0).astype(jnp.int32)
    return (live_count, partner, face_size)


def symmetric_blocks(seed_key, number_of, order, low, high, reach, target):

    def one_block(number):
        block_key = jax.random.fold_in(seed_key, number)
        noise = jax.random.normal(jax.random.fold_in(block_key, 1), (order, order), jnp.float32)
        coupling = (noise + noise.T) * (reach / (2.0 * math.sqrt(2.0 * order)))
        diagonal = jnp.exp(jax.random.uniform(jax.random.fold_in(block_key, 2), (order,), jnp.float32, math.log(low), math.log(high)))
        matrix = jnp.diag(diagonal) + coupling
        return matrix.astype(target)
    return lax.map(one_block, jnp.arange(number_of, dtype=jnp.int32))


def draw_slot_count(key, part):
    return layout_tables(key)[0]


def draw_partner(key, part):
    return layout_tables(key)[1]


def draw_face_size(key, part):
    return layout_tables(key)[2]


def draw_schur_matrix(key, part):
    blocks = symmetric_blocks(jax.random.fold_in(key, 11), SPACE * SLABS * SLOTS, NB, 1.5, 5.0, 1.2, jnp.bfloat16)
    return blocks.reshape(SPACE, SLABS, SLOTS, NB, NB)


def draw_face_inverse(key, part):
    blocks = symmetric_blocks(jax.random.fold_in(key, 23), SPACE * SLABS * SLOTS * NF, FW, 0.6, 1.5, 0.4, jnp.bfloat16)
    return blocks.reshape(SPACE, SLABS, SLOTS, NF, FW, FW)


def draw_coarse_group(key, part):
    return symmetric_blocks(jax.random.fold_in(key, 31), SPACE, NCG, 0.5, 2.0, 0.5, jnp.float32)


def draw_coarse_top(key, part):
    return symmetric_blocks(jax.random.fold_in(key, 37), 1, NT, 3.0, 6.0, 2.5, jnp.float32)[0]


def draw_deluxe(key, part):
    full_shape = (SPACE, SLABS, SLOTS, NF, FW, FW)
    noise = jax.random.normal(jax.random.fold_in(key, 41), full_shape, jnp.float32) * (0.35 / math.sqrt(FW))
    diagonal = jax.random.uniform(jax.random.fold_in(key, 43), full_shape[:-1], jnp.float32, 0.3, 0.8)
    identity = jnp.eye(FW, dtype=jnp.float32)
    return (noise + diagonal[..., None] * identity).astype(jnp.bfloat16)


def block_scale(stream_key, dims, shards, least, high):
    def one(position, parts):
        steps = jax.random.uniform(jax.random.fold_in(jax.random.fold_in(stream_key, 6), position), (parts,), jnp.float32, least / len(shards), high / len(shards))
        return jnp.repeat(jnp.exp(steps), dims[position] // parts).reshape((-1,) + (1,) * (len(dims) - position - 1))

    gain = one(*shards[0])
    for cut in shards[1:]:
        gain = gain * one(*cut)
    return gain


def scatter_about(own_key, shape, scale, bound, split=(), kind=jnp.bfloat16):
    drawn = scale * jax.random.normal(own_key, shape, jnp.float32)
    if split:
        drawn = drawn * block_scale(own_key, shape, split, -0.22, 0.18)
    return jnp.clip(drawn, -bound, bound).astype(kind)


def setup_inputs(seed: int = 0) -> dict:
    arg_keys = jax.random.split(jax.random.key(seed), 13)
    schur_matrix = draw_schur_matrix(jax.random.fold_in(arg_keys[12], 71), 0)
    face_inverse = draw_face_inverse(jax.random.fold_in(arg_keys[12], 71), 0)
    deluxe = draw_deluxe(jax.random.fold_in(arg_keys[12], 71), 0)
    primal_weight = jnp.clip(jnp.exp(math.log(0.3) - 1.7917595 * jax.random.uniform(arg_keys[3], (SPACE, SLABS, SLOTS, NF, FW), jnp.float32) ** block_scale(arg_keys[3], (SPACE, SLABS, SLOTS, NF, FW), ((0, 32), (1, 8)), -0.2, 0.2)), 0.05, 0.3)
    coarse_group = draw_coarse_group(jax.random.fold_in(arg_keys[12], 71), 0)
    coarse_map = scatter_about(arg_keys[5], (SPACE, NCG, NQ), NCG ** -0.5, 0.4375, ((0, 32), (1, 8)), jnp.float32)
    coarse_top = draw_coarse_top(jax.random.fold_in(arg_keys[12], 71), 0)
    load_vector = scatter_about(arg_keys[7], (SPACE, SLABS, SLOTS, NF, FW, NRHS), 1.0, 6.0, ((0, 32), (1, 8)))
    previous = scatter_about(arg_keys[8], (SPACE, SLABS, SLOTS, NF, FW, NRHS), 0.5, 3.0, ((0, 32), (1, 8)))
    slot_count = draw_slot_count(jax.random.fold_in(arg_keys[12], 71), 0)
    partner = draw_partner(jax.random.fold_in(arg_keys[12], 71), 0)
    face_size = draw_face_size(jax.random.fold_in(arg_keys[12], 71), 0)
    return {"schur_matrix": schur_matrix, "face_inverse": face_inverse, "deluxe": deluxe, "primal_weight": primal_weight, "coarse_group": coarse_group, "coarse_map": coarse_map, "coarse_top": coarse_top, "load_vector": load_vector, "previous": previous, "slot_count": slot_count, "partner": partner, "face_size": face_size}


precise = lax.Precision.HIGHEST


def live_entries(slot_count, face_size):
    slot_ids = jnp.arange(SLOTS, dtype=jnp.int32)
    entry_ids = jnp.arange(FW, dtype=jnp.int32)
    slot_alive = slot_ids[None, None, :] < slot_count[:, :, None]
    inside = entry_ids[None, None, None, None, :] < face_size[:, :, :, :, None]
    both_live = jnp.logical_and(slot_alive[:, :, :, None, None], inside)
    return jnp.where(both_live, 1.0, 0.0).astype(jnp.float32)[..., None]


def partner_values(values, partner):
    zero_slab = jnp.zeros_like(values[:, :1, :, 0])
    from_below = jnp.concatenate([zero_slab, values[:, :-1, :, 1]], axis=1)
    from_above = jnp.concatenate([values[:, 1:, :, 0], zero_slab], axis=1)
    from_left = jnp.roll(values[:, :, :, 3], 1, axis=0)
    from_right = jnp.roll(values[:, :, :, 2], -1, axis=0)
    sources = jnp.stack([from_below, from_above, from_left, from_right, values[:, :, :, 5], values[:, :, :, 4], values[:, :, :, 7], values[:, :, :, 6]], axis=3)
    chosen = jnp.clip(partner, 0, SLOTS - 1).astype(jnp.int32)
    picked = jnp.take_along_axis(sources, chosen[:, :, :, :, None, None], axis=2)
    return jnp.where((partner >= 0)[:, :, :, :, None, None], picked, jnp.zeros_like(picked))


def apply_schur(schur_matrix, direction_half):
    blocks = schur_matrix.reshape(SPACE * SLABS * SLOTS, NB, NB)
    vectors = direction_half.reshape(SPACE * SLABS * SLOTS, NB, NRHS)

    def product(operands):
        return jnp.dot(operands[0], operands[1], preferred_element_type=jnp.float32)

    return lax.map(product, (blocks, vectors)).reshape(direction_half.shape)


def reference(schur_matrix, face_inverse, deluxe, primal_weight, coarse_group, coarse_map, coarse_top, load_vector, previous, slot_count, partner, face_size):
    live_mask = live_entries(slot_count, face_size)
    linked = (partner >= 0)[:, :, :, :, None, None]
    shared = jnp.where(linked, 0.5, 1.0).astype(jnp.float32)
    deluxe_full = deluxe.astype(jnp.float32)
    inverse_full = face_inverse.astype(jnp.float32)

    def assemble(values):
        return values + partner_values(values, partner)

    def global_inner(first_vec, second_vec):
        return jnp.sum(shared * first_vec * second_vec, axis=(0, 1, 2, 3, 4))

    def operator(values):
        return live_mask * apply_schur(schur_matrix, values.astype(jnp.bfloat16))

    def precondition(values):
        res_half = values.astype(jnp.bfloat16).astype(jnp.float32)
        scaled = live_mask * jnp.einsum("wnsfkj,wnsfkr->wnsfjr", deluxe_full, res_half)
        scaled_half = scaled.astype(jnp.bfloat16).astype(jnp.float32)
        local_part = jnp.einsum("wnsfjk,wnsfkr->wnsfjr", inverse_full, scaled_half)
        coarse_in = jnp.sum(primal_weight[..., None] * scaled, axis=4)
        group_vec = coarse_in.reshape(SPACE, NCG, NRHS)
        group_part = jnp.einsum("wcd,wdr->wcr", coarse_group, group_vec, precision=precise)
        restricted = jnp.einsum("wcq,wcr->wqr", coarse_map, group_vec, precision=precise).reshape(NT, NRHS)
        top_part = jnp.dot(coarse_top, restricted, precision=precise).reshape(SPACE, NQ, NRHS)
        coarse_out = group_part + jnp.einsum("wcq,wqr->wcr", coarse_map, top_part, precision=precise)
        coarse_out = coarse_out.reshape(SPACE, SLABS, SLOTS, NF, 1, NRHS)
        correction = local_part + primal_weight[..., None] * coarse_out
        corr_half = (live_mask * correction).astype(jnp.bfloat16).astype(jnp.float32)
        weighted = live_mask * jnp.einsum("wnsfjk,wnsfkr->wnsfjr", deluxe_full, corr_half)
        return assemble(weighted)

    prev_full = previous.astype(jnp.float32)
    prev_partner = partner_values(previous, partner).astype(jnp.float32)
    averaged = live_mask * jnp.where(linked, 0.5 * (prev_full + prev_partner), prev_full)
    residual = assemble(live_mask * load_vector.astype(jnp.float32) - operator(averaged))
    solution = averaged
    precond = precondition(residual)
    precond_norm = global_inner(residual, precond)
    direction = precond
    for iteration in range(ITERS):
        image_full = assemble(operator(direction))
        step_size = precond_norm / global_inner(direction, image_full)
        solution = solution + step_size * direction
        residual = residual - step_size * image_full
        if iteration + 1 < ITERS:
            precond = precondition(residual)
            next_norm = global_inner(residual, precond)
            direction = precond + (next_norm / precond_norm) * direction
            precond_norm = next_norm
    return solution, residual
```

```python
import functools

import jax
import jax.numpy as jnp
from jax import lax
from jax.experimental import pallas as pl
from jax.experimental.pallas import tpu as pltpu
from jax.sharding import PartitionSpec as P

ITERS = 2
SLOTS = 3
NF = 8
FW = 128
NB = NF * FW
MESH = pl.DeviceIdType.MESH
HIGH = lax.Precision.HIGHEST
F32 = jnp.float32
BF16 = jnp.bfloat16
EXCHANGES = 2 * ITERS + 1
REDUCES = 2 * ITERS - 1


def kernel(
    wide,
    narrow,
    schur_in,
    inverse_in,
    deluxe_in,
    weight_in,
    group_ref,
    map_ref,
    top_ref,
    load_in,
    previous_in,
    count_ref,
    partner_ref,
    size_ref,
    solution_out,
    residual_out,
    schur,
    inverse,
    deluxe,
    load,
    previous,
    turned,
    weight,
    sol,
    res,
    direc,
    image,
    weighted,
    local,
    half,
    scaled_half,
    coarse,
    got_half,
    got_0,
    got_1,
    got_2,
    got_3,
    got_4,
    vec_buf,
    part_buf,
    every_buf,
    plane_buf,
    line_buf,
    load_sem,
    half_send,
    half_recv,
    face_send,
    face_recv,
    vec_send,
    vec_recv,
    part_send,
    part_recv,
    every_send,
    every_recv,
    plane_send,
    plane_recv,
    line_send,
    line_recv,
    out_sem,
):
    got = (got_0, got_1, got_2, got_3, got_4)
    w = lax.axis_index("wide")
    n = lax.axis_index("narrow")

    loads = [
        pltpu.make_async_copy(previous_in, previous, load_sem.at[0]),
        pltpu.make_async_copy(deluxe_in, deluxe, load_sem.at[1]),
        pltpu.make_async_copy(schur_in, schur, load_sem.at[2]),
        pltpu.make_async_copy(load_in, load, load_sem.at[3]),
        pltpu.make_async_copy(inverse_in, inverse, load_sem.at[4]),
    ]
    for copy in loads:
        copy.start()

    barrier = pltpu.get_barrier_semaphore()

    def greet_wide(d, carry):
        pl.semaphore_signal(
            barrier, inc=1, device_id=(lax.rem(w + d, wide), n), device_id_type=MESH
        )
        return carry

    def greet_narrow(d, carry):
        pl.semaphore_signal(
            barrier, inc=1, device_id=(w, lax.rem(n + d, narrow)), device_id_type=MESH
        )
        return carry

    lax.fori_loop(1, wide, greet_wide, 0)
    lax.fori_loop(1, narrow, greet_narrow, 0)

    rows = lax.broadcasted_iota(jnp.int32, (FW, FW), 0)
    count = count_ref[0, 0]

    def inside(s, f):
        size = jnp.where(s < count, size_ref[s, f], 0)
        return rows < size

    def masked(s, f, values):
        return jnp.where(inside(s, f), values, 0.0)

    def picked(values, arrived, s, f):
        t = partner_ref[s, f]
        slot = jnp.maximum(t, 0)
        source = arrived[f, slot] if f < 4 else values[slot, f ^ 1]
        return jnp.where(t >= 0, source.astype(F32), 0.0)

    def face_copies(values, arrived, send, recv, s):
        return [
            pltpu.make_async_remote_copy(
                src_ref=values.at[s, f],
                dst_ref=arrived.at[to, s],
                send_sem=send.at[to],
                recv_sem=recv.at[to],
                device_id=device,
                device_id_type=MESH,
            )
            for f, to, device in (
                (1, 0, (w, lax.rem(n + 1, narrow))),
                (0, 1, (w, lax.rem(n + narrow - 1, narrow))),
                (3, 2, (lax.rem(w + 1, wide), n)),
                (2, 3, (lax.rem(w + wide - 1, wide), n)),
            )
        ]

    def send_faces(values, arrived, send, recv, s):
        up, down, right, left = face_copies(values, arrived, send, recv, s)

        @pl.when(n < narrow - 1)
        def _():
            up.start()

        @pl.when(n > 0)
        def _():
            down.start()

        right.start()
        left.start()

    def wait_bytes(ref, sem):
        pltpu.make_async_copy(ref, ref, sem).wait()

    def wait_faces(arrived, recv):
        @pl.when(n > 0)
        def _():
            wait_bytes(arrived.at[0], recv.at[0])

        @pl.when(n < narrow - 1)
        def _():
            wait_bytes(arrived.at[1], recv.at[1])

        wait_bytes(arrived.at[2], recv.at[2])
        wait_bytes(arrived.at[3], recv.at[3])

    def wait_sent(arrived, send):
        @pl.when(n < narrow - 1)
        def _():
            wait_bytes(arrived.at[0], send.at[0])

        @pl.when(n > 0)
        def _():
            wait_bytes(arrived.at[1], send.at[1])

        wait_bytes(arrived.at[2], send.at[2])
        wait_bytes(arrived.at[3], send.at[3])

    def spread_narrow(buf, send, recv):
        def one(d, carry):
            pltpu.make_async_remote_copy(
                src_ref=buf.at[n],
                dst_ref=buf.at[n],
                send_sem=send,
                recv_sem=recv,
                device_id=(w, lax.rem(n + d, narrow)),
                device_id_type=MESH,
            ).start()
            return carry

        lax.fori_loop(1, narrow, one, 0)

    def spread_wide(buf, send, recv):
        def one(d, carry):
            pltpu.make_async_remote_copy(
                src_ref=buf.at[w],
                dst_ref=buf.at[w],
                send_sem=send,
                recv_sem=recv,
                device_id=(lax.rem(w + d, wide), n),
                device_id_type=MESH,
            ).start()
            return carry

        lax.fori_loop(1, wide, one, 0)

    def wait_spread(buf, sem):
        wait_bytes(buf.at[pl.ds(0, buf.shape[0] - 1)], sem)

    def fold(product):
        return jnp.sum(product.reshape(FW // 8, 8, FW), axis=0)

    def reduce_start(k, first, second):
        plane_buf[k, w] = jnp.concatenate(
            [jnp.sum(first, axis=0, keepdims=True), jnp.sum(second, axis=0, keepdims=True)], axis=0
        )
        spread_wide(plane_buf.at[k], plane_send.at[k], plane_recv.at[k])

    def reduce_middle(k):
        wait_spread(plane_buf.at[k], plane_recv.at[k])
        line_buf[k, n] = jnp.sum(plane_buf[k], axis=0)
        spread_narrow(line_buf.at[k], line_send.at[k], line_recv.at[k])

    def reduce_end(k):
        wait_spread(line_buf.at[k], line_recv.at[k])
        total = jnp.sum(line_buf[k], axis=0)
        return total[0:1], total[1:2]

    def spread_weight(s, carry):
        for f in range(NF):
            row = weight_in[s, f : f + 1, :]
            column = jnp.broadcast_to(row, (FW, FW)).T
            weight[s, f] = masked(s, f, column)
        return carry

    lax.fori_loop(0, SLOTS, spread_weight, 0)
    loads[1].wait()

    def turn(s, carry):
        for f in range(NF):
            turned[s, f] = deluxe[s, f].T
        return carry

    lax.fori_loop(0, SLOTS, turn, 0)
    loads[0].wait()
    pl.semaphore_wait(barrier, wide + narrow - 2)

    for s in range(SLOTS):
        send_faces(previous, got_half, half_send, half_recv, s)
    wait_faces(got_half, half_recv)

    def average(s, carry):
        for f in range(NF):
            own = previous[s, f].astype(F32)
            across = picked(previous, got_half, s, f)
            mean = jnp.where(partner_ref[s, f] >= 0, 0.5 * (own + across), own)
            mean = masked(s, f, mean)
            sol[s, f] = mean
            half[s, pl.ds(f * FW, FW), :] = mean.astype(BF16)
        return carry

    lax.fori_loop(0, SLOTS, average, 0)
    loads[2].wait()
    loads[3].wait()

    def start_residual(s, carry):
        product = jnp.dot(schur[s], half[s], preferred_element_type=F32)
        for f in range(NF):
            image[s, f] = masked(
                s, f, load[s, f].astype(F32) - product[f * FW : (f + 1) * FW]
            )
        send_faces(image, got[0], face_send.at[0], face_recv.at[0], s)
        return carry

    lax.fori_loop(0, SLOTS, start_residual, 0)
    loads[4].wait()
    zero = jnp.zeros((8, FW), F32)

    def scaled_of(m, s, f, values):
        scaled = masked(
            s, f, jnp.dot(turned[s, f], values.astype(BF16), preferred_element_type=F32)
        )
        scaled_half[s, f] = scaled.astype(BF16)
        return jnp.sum(fold(weight[s, f] * scaled), axis=0, keepdims=True)

    def coarse_start(m):
        entering = vec_buf[m, n]
        part_buf[m, n] = lax.dot_general(
            map_ref[...], entering, (((0,), (0,)), ((), ())), precision=HIGH
        )
        spread_narrow(part_buf.at[m], part_send.at[m], part_recv.at[m])
        spread_narrow(vec_buf.at[m], vec_send.at[m], vec_recv.at[m])

    def local_parts():
        def one(s, carry):
            for f in range(NF):
                local[s, f] = masked(
                    s, f, jnp.dot(inverse[s, f], scaled_half[s, f], preferred_element_type=F32)
                )
            return carry

        lax.fori_loop(0, SLOTS, one, 0)

    def coarse_end(m):
        wait_spread(part_buf.at[m], part_recv.at[m])
        every_buf[m, w] = jnp.sum(part_buf[m], axis=0)
        spread_wide(every_buf.at[m], every_send.at[m], every_recv.at[m])
        wait_spread(vec_buf.at[m], vec_recv.at[m])
        group = jnp.dot(
            group_ref[...], vec_buf[m].reshape(narrow * SLOTS * NF, FW), precision=HIGH
        )
        wait_spread(every_buf.at[m], every_recv.at[m])
        top = jnp.dot(top_ref[...], every_buf[m].reshape(wide * 8, FW), precision=HIGH)
        coarse[...] = group + jnp.dot(map_ref[...], top, precision=HIGH)

    def weigh(e, send_now):
        def one(s, total):
            for f in range(NF):
                out = coarse[pl.ds(s * NF + f, 1), :]
                correction = (local[s, f] + weight[s, f] * out).astype(BF16)
                value = masked(
                    s, f, jnp.dot(deluxe[s, f], correction, preferred_element_type=F32)
                )
                weighted[s, f] = value
                total = total + fold(res[s, f] * value)
            if send_now:
                send_faces(weighted, got[e], face_send.at[e], face_recv.at[e], s)
            return total

        return lax.fori_loop(0, SLOTS, one, zero)

    def operate(e):
        def one(s, total):
            product = jnp.dot(schur[s], half[s], preferred_element_type=F32)
            for f in range(NF):
                value = masked(s, f, product[f * FW : (f + 1) * FW])
                image[s, f] = value
                total = total + fold(direc[s, f] * value)
            return total

        return lax.fori_loop(0, SLOTS, one, zero)

    def send_all(values, e):
        def one(s, carry):
            send_faces(values, got[e], face_send.at[e], face_recv.at[e], s)
            return carry

        lax.fori_loop(0, SLOTS, one, 0)

    wait_faces(got[0], face_recv.at[0])

    def first_residual(s, carry):
        primal = []
        for f in range(NF):
            value = image[s, f] + picked(image, got[0], s, f)
            res[s, f] = value
            primal.append(scaled_of(0, s, f, value))
        vec_buf[0, n, pl.ds(s * NF, NF), :] = jnp.concatenate(primal, axis=0)
        return carry

    lax.fori_loop(0, SLOTS, first_residual, 0)
    coarse_start(0)
    local_parts()
    coarse_end(0)
    norm_part = weigh(1, True)
    wait_faces(got[1], face_recv.at[1])

    def first_direction(s, carry):
        for f in range(NF):
            value = weighted[s, f] + picked(weighted, got[1], s, f)
            direc[s, f] = value
            half[s, pl.ds(f * FW, FW), :] = value.astype(BF16)
        return carry

    lax.fori_loop(0, SLOTS, first_direction, 0)
    wait_sent(got[0], face_send.at[0])
    curve_part = operate(2)
    reduce_start(0, norm_part, curve_part)
    send_all(image, 2)
    reduce_middle(0)
    wait_faces(got[2], face_recv.at[2])
    norm, curve = reduce_end(0)
    step = norm / curve

    def next_residual(s, carry):
        primal = []
        for f in range(NF):
            full = image[s, f] + picked(image, got[2], s, f)
            value = res[s, f] - step * full
            res[s, f] = value
            primal.append(scaled_of(1, s, f, value))
        vec_buf[1, n, pl.ds(s * NF, NF), :] = jnp.concatenate(primal, axis=0)
        return carry

    lax.fori_loop(0, SLOTS, next_residual, 0)
    coarse_start(1)
    local_parts()

    def next_solution(s, carry):
        for f in range(NF):
            sol[s, f] = sol[s, f] + step * direc[s, f]
        return carry

    lax.fori_loop(0, SLOTS, next_solution, 0)
    wait_sent(got[1], face_send.at[1])
    coarse_end(1)
    norm_part = weigh(3, False)
    reduce_start(1, norm_part, norm_part)
    send_all(weighted, 3)
    reduce_middle(1)
    wait_faces(got[3], face_recv.at[3])
    following, _ = reduce_end(1)
    ratio = following / norm

    def next_direction(s, carry):
        for f in range(NF):
            value = weighted[s, f] + picked(weighted, got[3], s, f)
            value = value + ratio * direc[s, f]
            direc[s, f] = value
            half[s, pl.ds(f * FW, FW), :] = value.astype(BF16)
        return carry

    lax.fori_loop(0, SLOTS, next_direction, 0)
    wait_sent(got[2], face_send.at[2])
    curve_part = operate(4)
    reduce_start(2, curve_part, curve_part)
    send_all(image, 4)
    reduce_middle(2)
    wait_faces(got[4], face_recv.at[4])

    def last_image(s, carry):
        for f in range(NF):
            local[s, f] = image[s, f] + picked(image, got[4], s, f)
        return carry

    lax.fori_loop(0, SLOTS, last_image, 0)
    curve, _ = reduce_end(2)
    step = following / curve
    outs = []
    for s in range(SLOTS):
        for f in range(NF):
            sol[s, f] = sol[s, f] + step * direc[s, f]
        outs.append(pltpu.make_async_copy(sol.at[s], solution_out.at[s], out_sem.at[0, s]))
        outs[-1].start()
        for f in range(NF):
            res[s, f] = res[s, f] - step * local[s, f]
        outs.append(pltpu.make_async_copy(res.at[s], residual_out.at[s], out_sem.at[1, s]))
        outs[-1].start()

    wait_sent(got_half, half_send)
    wait_sent(got[3], face_send.at[3])
    wait_sent(got[4], face_send.at[4])
    for m in range(ITERS):
        wait_spread(part_buf.at[m], part_send.at[m])
        wait_spread(vec_buf.at[m], vec_send.at[m])
        wait_spread(every_buf.at[m], every_send.at[m])
    for k in range(REDUCES):
        wait_spread(plane_buf.at[k], plane_send.at[k])
        wait_spread(line_buf.at[k], line_send.at[k])
    for copy in outs:
        copy.wait()


def solution(mesh):
    wide, narrow = mesh.shape["wide"], mesh.shape["narrow"]
    faces = (SLOTS, NF, FW, FW)
    dma = pltpu.SemaphoreType.DMA

    def body(
        schur_matrix,
        face_inverse,
        deluxe,
        primal_weight,
        coarse_group,
        coarse_map,
        coarse_top,
        load_vector,
        previous,
        slot_count,
        partner,
        face_size,
    ):
        far = pl.BlockSpec(memory_space=pl.ANY)
        near = pl.BlockSpec(memory_space=pltpu.VMEM)
        scalar = pl.BlockSpec(memory_space=pltpu.SMEM)
        sol, res = pl.pallas_call(
            functools.partial(kernel, wide, narrow),
            out_shape=[jax.ShapeDtypeStruct(faces, F32)] * 2,
            in_specs=[far, far, far, near, near, near, near, far, far, scalar, scalar, scalar],
            out_specs=[far, far],
            scratch_shapes=[
                pltpu.VMEM((SLOTS, NB, NB), BF16),
                pltpu.VMEM(faces, BF16),
                pltpu.VMEM(faces, BF16),
                pltpu.VMEM(faces, BF16),
                pltpu.VMEM(faces, BF16),
                pltpu.VMEM(faces, BF16),
                pltpu.VMEM(faces, F32),
                pltpu.VMEM(faces, F32),
                pltpu.VMEM(faces, F32),
                pltpu.VMEM(faces, F32),
                pltpu.VMEM(faces, F32),
                pltpu.VMEM(faces, F32),
                pltpu.VMEM(faces, F32),
                pltpu.VMEM((SLOTS, NB, FW), BF16),
                pltpu.VMEM(faces, BF16),
                pltpu.VMEM((SLOTS * NF, FW), F32),
                pltpu.VMEM((4, SLOTS, FW, FW), BF16),
                *[pltpu.VMEM((4, SLOTS, FW, FW), F32)] * EXCHANGES,
                pltpu.VMEM((ITERS, narrow, SLOTS * NF, FW), F32),
                pltpu.VMEM((ITERS, narrow, 8, FW), F32),
                pltpu.VMEM((ITERS, wide, 8, FW), F32),
                pltpu.VMEM((REDUCES, wide, 2, FW), F32),
                pltpu.VMEM((REDUCES, narrow, 2, FW), F32),
                dma((5,)),
                dma((4,)),
                dma((4,)),
                dma((EXCHANGES, 4)),
                dma((EXCHANGES, 4)),
                dma((ITERS,)),
                dma((ITERS,)),
                dma((ITERS,)),
                dma((ITERS,)),
                dma((ITERS,)),
                dma((ITERS,)),
                dma((REDUCES,)),
                dma((REDUCES,)),
                dma((REDUCES,)),
                dma((REDUCES,)),
                dma((2, SLOTS)),
            ],
            compiler_params=pltpu.CompilerParams(
                collective_id=0, has_side_effects=True, vmem_limit_bytes=60 * 1024 * 1024
            ),
        )(
            schur_matrix[0, 0],
            face_inverse[0, 0],
            deluxe[0, 0],
            primal_weight[0, 0],
            coarse_group[0],
            coarse_map[0],
            coarse_top,
            load_vector[0, 0],
            previous[0, 0],
            slot_count,
            partner[0, 0],
            face_size[0, 0],
        )
        return sol[None, None], res[None, None]

    both = ("wide", "narrow")
    deep = P(*both, None, None, None, None)
    return jax.shard_map(
        body,
        mesh=mesh,
        in_specs=(
            P(*both, None, None, None),
            deep,
            deep,
            P(*both, None, None, None),
            P(*both, None),
            P(*both, None),
            P("wide", None),
            deep,
            deep,
            P(*both),
            P(*both, None, None),
            P(*both, None, None),
        ),
        out_specs=(deep, deep),
        check_vma=False,
    )
```

```python
import functools

import jax
import jax.numpy as jnp
from jax import lax
from jax.experimental import pallas as pl
from jax.experimental.pallas import tpu as pltpu
from jax.sharding import PartitionSpec as P

ITERS = 2
SLOTS = 3
NF = 8
FW = 128
NB = NF * FW
MESH = pl.DeviceIdType.MESH
HIGH = lax.Precision.HIGHEST
F32 = jnp.float32
BF16 = jnp.bfloat16
EXCHANGES = ITERS + 1
REDUCES = 2 * ITERS - 1


def kernel(
    wide,
    narrow,
    schur_in,
    inverse_in,
    deluxe_in,
    weight_in,
    group_ref,
    map_ref,
    top_ref,
    load_in,
    previous_in,
    count_ref,
    partner_ref,
    size_ref,
    sol,
    direc,
    res,
    full,
    step_out,
    schur,
    inverse,
    deluxe,
    load,
    previous,
    turned,
    weight,
    image,
    weighted,
    local,
    lift,
    over_deluxe,
    over_inverse,
    over_turned,
    over_weight,
    over_local,
    half,
    scaled_half,
    coarse,
    group,
    third,
    top_buf,
    got_half,
    got_0,
    got_1,
    got_2,
    rows_out,
    rows_0,
    rows_1,
    rows_2,
    vec_buf,
    part_buf,
    every_buf,
    plane_buf,
    line_buf,
    load_sem,
    half_send,
    half_recv,
    face_send,
    face_recv,
    vec_send,
    vec_recv,
    part_send,
    part_recv,
    every_send,
    every_recv,
    plane_send,
    plane_recv,
    line_send,
    line_recv,
    top_send,
    top_recv,
    over_send,
    over_recv,
    rows_send,
    rows_recv,
):
    got = (got_0, got_1, got_2)
    rows_got = (rows_0, rows_1, rows_2)
    w = lax.axis_index("wide")
    n = lax.axis_index("narrow")

    loads = [
        pltpu.make_async_copy(previous_in, previous, load_sem.at[0]),
        pltpu.make_async_copy(deluxe_in, deluxe, load_sem.at[1]),
        pltpu.make_async_copy(schur_in, schur, load_sem.at[2]),
        pltpu.make_async_copy(load_in, load, load_sem.at[3]),
        pltpu.make_async_copy(inverse_in, inverse, load_sem.at[4]),
    ]
    for copy in loads:
        copy.start()

    barrier = pltpu.get_barrier_semaphore()

    def greet_wide(d, carry):
        pl.semaphore_signal(
            barrier, inc=1, device_id=(lax.rem(w + d, wide), n), device_id_type=MESH
        )
        return carry

    def greet_narrow(d, carry):
        pl.semaphore_signal(
            barrier, inc=1, device_id=(w, lax.rem(n + d, narrow)), device_id_type=MESH
        )
        return carry

    lax.fori_loop(1, wide, greet_wide, 0)
    lax.fori_loop(1, narrow, greet_narrow, 0)

    rows = lax.broadcasted_iota(jnp.int32, (FW, FW), 0)
    count = count_ref[0, 0]

    def inside(s, f):
        size = jnp.where(s < count, size_ref[s, 0, f], 0)
        return rows < size

    def masked(s, f, values):
        return jnp.where(inside(s, f), values, 0.0)

    def picked(values, arrived, s, f):
        t = partner_ref[s, 0, f]
        slot = jnp.maximum(t, 0)
        source = arrived[f, slot] if f < 4 else values[slot, f ^ 1]
        return jnp.where(t >= 0, source.astype(F32), 0.0)

    def face_copies(values, arrived, send, recv, s):
        return [
            pltpu.make_async_remote_copy(
                src_ref=values.at[s, f],
                dst_ref=arrived.at[to, s],
                send_sem=send.at[to],
                recv_sem=recv.at[to],
                device_id=device,
                device_id_type=MESH,
            )
            for f, to, device in (
                (1, 0, (w, lax.rem(n + 1, narrow))),
                (0, 1, (w, lax.rem(n + narrow - 1, narrow))),
                (3, 2, (lax.rem(w + 1, wide), n)),
                (2, 3, (lax.rem(w + wide - 1, wide), n)),
            )
        ]

    def send_faces(values, arrived, send, recv, s):
        up, down, right, left = face_copies(values, arrived, send, recv, s)

        @pl.when(n < narrow - 1)
        def _():
            up.start()

        @pl.when(n > 0)
        def _():
            down.start()

        right.start()
        left.start()

    def send_rows(i, row_of):
        for to, f in ((0, 1), (1, 0), (2, 3), (3, 2)):
            rows_out[i, to] = jnp.concatenate(
                [row_of(s, f) for s in range(SLOTS)] + [jnp.zeros((8 - SLOTS, FW), F32)], axis=0
            )
        up, down, right, left = [
            pltpu.make_async_remote_copy(
                src_ref=rows_out.at[i, to],
                dst_ref=rows_got[i].at[to],
                send_sem=rows_send.at[i, to],
                recv_sem=rows_recv.at[i, to],
                device_id=device,
                device_id_type=MESH,
            )
            for to, device in enumerate(
                (
                    (w, lax.rem(n + 1, narrow)),
                    (w, lax.rem(n + narrow - 1, narrow)),
                    (lax.rem(w + 1, wide), n),
                    (lax.rem(w + wide - 1, wide), n),
                )
            )
        ]

        @pl.when(n < narrow - 1)
        def _():
            up.start()

        @pl.when(n > 0)
        def _():
            down.start()

        right.start()
        left.start()

    def wait_bytes(ref, sem):
        pltpu.make_async_copy(ref, ref, sem).wait()

    def wait_faces(arrived, recv):
        @pl.when(n > 0)
        def _():
            wait_bytes(arrived.at[0], recv.at[0])

        @pl.when(n < narrow - 1)
        def _():
            wait_bytes(arrived.at[1], recv.at[1])

        wait_bytes(arrived.at[2], recv.at[2])
        wait_bytes(arrived.at[3], recv.at[3])

    def wait_sent(arrived, send):
        @pl.when(n < narrow - 1)
        def _():
            wait_bytes(arrived.at[0], send.at[0])

        @pl.when(n > 0)
        def _():
            wait_bytes(arrived.at[1], send.at[1])

        wait_bytes(arrived.at[2], send.at[2])
        wait_bytes(arrived.at[3], send.at[3])

    def spread_narrow(buf, send, recv):
        def one(d, carry):
            pltpu.make_async_remote_copy(
                src_ref=buf.at[n],
                dst_ref=buf.at[n],
                send_sem=send,
                recv_sem=recv,
                device_id=(w, lax.rem(n + d, narrow)),
                device_id_type=MESH,
            ).start()
            return carry

        lax.fori_loop(1, narrow, one, 0)

    def spread_wide(buf, send, recv):
        def one(d, carry):
            pltpu.make_async_remote_copy(
                src_ref=buf.at[w],
                dst_ref=buf.at[w],
                send_sem=send,
                recv_sem=recv,
                device_id=(lax.rem(w + d, wide), n),
                device_id_type=MESH,
            ).start()
            return carry

        lax.fori_loop(1, wide, one, 0)

    def wait_spread(buf, sem):
        wait_bytes(buf.at[pl.ds(0, buf.shape[0] - 1)], sem)

    def fold(product):
        return jnp.sum(product.reshape(FW // 8, 8, FW), axis=0)

    def reduce_start(k, first, second):
        plane_buf[k, w] = jnp.concatenate(
            [jnp.sum(first, axis=0, keepdims=True), jnp.sum(second, axis=0, keepdims=True)], axis=0
        )
        spread_wide(plane_buf.at[k], plane_send.at[k], plane_recv.at[k])

    def reduce_middle(k):
        wait_spread(plane_buf.at[k], plane_recv.at[k])
        line_buf[k, n] = jnp.sum(plane_buf[k], axis=0)
        spread_narrow(line_buf.at[k], line_send.at[k], line_recv.at[k])

    def reduce_end(k):
        wait_spread(line_buf.at[k], line_recv.at[k])
        total = jnp.sum(line_buf[k], axis=0)
        return total[0:1], total[1:2]

    def spread_weight(s, carry):
        for f in range(NF):
            row = weight_in[s, f : f + 1, :]
            column = jnp.broadcast_to(row, (FW, FW)).T
            weight[s, f] = masked(s, f, column)
        return carry

    lax.fori_loop(0, SLOTS, spread_weight, 0)
    loads[1].wait()

    def turn(s, carry):
        for f in range(NF):
            turned[s, f] = deluxe[s, f].T
        return carry

    lax.fori_loop(0, SLOTS, turn, 0)
    loads[0].wait()
    pl.semaphore_wait(barrier, wide + narrow - 2)

    for s in range(SLOTS):
        send_faces(previous, got_half, half_send, half_recv, s)
    send_rows(ITERS, lambda s, f: weight_in[s, f : f + 1, :])
    for s in range(SLOTS):
        send_faces(deluxe, over_deluxe, over_send.at[0], over_recv.at[0], s)
    loads[4].wait()
    for s in range(SLOTS):
        send_faces(inverse, over_inverse, over_send.at[1], over_recv.at[1], s)
    top_buf[w] = top_ref[...]
    spread_wide(top_buf, top_send, top_recv)
    wait_faces(got_half, half_recv)

    def average(s, carry):
        for f in range(NF):
            own = previous[s, f].astype(F32)
            across = picked(previous, got_half, s, f)
            mean = jnp.where(partner_ref[s, 0, f] >= 0, 0.5 * (own + across), own)
            mean = masked(s, f, mean)
            sol[s, f] = mean
            half[s, pl.ds(f * FW, FW), :] = mean.astype(BF16)
        return carry

    lax.fori_loop(0, SLOTS, average, 0)
    loads[2].wait()
    loads[3].wait()

    def start_residual(s, carry):
        product = jnp.dot(schur[s], half[s], preferred_element_type=F32)
        for f in range(NF):
            image[s, f] = masked(
                s, f, load[s, f].astype(F32) - product[f * FW : (f + 1) * FW]
            )
        send_faces(image, got[0], face_send.at[0], face_recv.at[0], s)
        return carry

    lax.fori_loop(0, SLOTS, start_residual, 0)
    zero = jnp.zeros((8, FW), F32)

    def scaled_of(s, f, values):
        scaled = masked(
            s, f, jnp.dot(turned[s, f], values.astype(BF16), preferred_element_type=F32)
        )
        scaled_half[s, f] = scaled.astype(BF16)
        return scaled

    def column_sum(values):
        return jnp.sum(values, axis=0, keepdims=True)

    def coarse_start(m):
        entering = vec_buf[m, n]
        part_buf[m, n] = jnp.dot(map_ref[...], entering, precision=HIGH)
        spread_narrow(part_buf.at[m], part_send.at[m], part_recv.at[m])
        spread_narrow(vec_buf.at[m], vec_send.at[m], vec_recv.at[m])

    def local_parts():
        def one(s, total):
            for f in range(NF):
                entering = scaled_half[s, f]
                value = masked(
                    s, f, jnp.dot(inverse[s, f], entering, preferred_element_type=F32)
                )
                local[s, f] = value
                total = total + fold(entering.astype(F32) * value)
            return total

        return lax.fori_loop(0, SLOTS, one, zero)

    def over_tables(s, carry):
        for f in range(4):
            slot = jnp.maximum(partner_ref[s, 0, f], 0)
            over_turned[s, f] = over_deluxe[f, slot].T
            row = rows_2[f, pl.ds(slot, 1), :]
            over_weight[s, f] = masked(s, f, jnp.broadcast_to(row, (FW, FW)).T)
        return carry

    def over_parts():
        def one(s, carry):
            for f in range(4):
                slot = jnp.maximum(partner_ref[s, 0, f], 0)
                scaled = masked(
                    s,
                    f,
                    jnp.dot(
                        over_turned[s, f], res[s, f].astype(BF16), preferred_element_type=F32
                    ),
                )
                over_local[s, f] = masked(
                    s,
                    f,
                    jnp.dot(
                        over_inverse[f, slot], scaled.astype(BF16), preferred_element_type=F32
                    ),
                )
            return carry

        lax.fori_loop(0, SLOTS, one, 0)

    def across_weighted(m, s, f):
        t = partner_ref[s, 0, f]
        slot = jnp.maximum(t, 0)
        if f < 4:
            out = rows_got[m][f, pl.ds(slot, 1), :]
            correction = (over_local[s, f] + over_weight[s, f] * out).astype(BF16)
            value = masked(
                s, f, jnp.dot(over_deluxe[f, slot], correction, preferred_element_type=F32)
            )
        else:
            value = weighted[slot, f ^ 1]
        return jnp.where(t >= 0, value, 0.0)

    def coarse_row(s, f):
        return coarse[s * NF + f : s * NF + f + 1, :]

    def wait_rows(i):
        wait_faces(rows_got[i], rows_recv.at[i])

    def make_lift(s, carry):
        for f in range(NF):
            value = weight[s, f]
            main = value.astype(BF16)
            rest = (value - main.astype(F32)).astype(BF16)
            lift[s, f] = jnp.dot(deluxe[s, f], main, preferred_element_type=F32) + jnp.dot(
                deluxe[s, f], rest, preferred_element_type=F32
            )
        return carry

    def coarse_middle(m):
        wait_spread(part_buf.at[m], part_recv.at[m])
        every_buf[m, w] = jnp.sum(part_buf[m], axis=0)
        spread_wide(every_buf.at[m], every_send.at[m], every_recv.at[m])
        wait_spread(vec_buf.at[m], vec_recv.at[m])
        group[m] = jnp.dot(
            group_ref[...], vec_buf[m].reshape(narrow * SLOTS * NF, FW), precision=HIGH
        )

    def coarse_end(m):
        wait_spread(every_buf.at[m], every_recv.at[m])
        third[m] = jnp.dot(
            top_buf[...].reshape(wide * 8, wide * 8),
            every_buf[m].reshape(wide * 8, FW),
            precision=HIGH,
        )
        own = third[m, pl.ds(pl.multiple_of(w * 8, 8), 8), :]
        return group[m] + lax.dot_general(
            map_ref[...], own, (((0,), (0,)), ((), ())), precision=HIGH
        )

    def weigh():
        def one(s, total):
            for f in range(NF):
                out = coarse[pl.ds(s * NF + f, 1), :]
                correction = (local[s, f] + weight[s, f] * out).astype(BF16)
                value = masked(
                    s, f, jnp.dot(deluxe[s, f], correction, preferred_element_type=F32)
                )
                weighted[s, f] = value
                total = total + fold(res[s, f] * value)
            return total

        return lax.fori_loop(0, SLOTS, one, zero)

    def operate():
        def one(s, total):
            product = jnp.dot(schur[s], half[s], preferred_element_type=F32)
            for f in range(NF):
                value = masked(s, f, product[f * FW : (f + 1) * FW])
                image[s, f] = value
                total = total + fold(direc[s, f] * value)
            return total

        return lax.fori_loop(0, SLOTS, one, zero)

    def send_all(values, e):
        def one(s, carry):
            send_faces(values, got[e], face_send.at[e], face_recv.at[e], s)
            return carry

        lax.fori_loop(0, SLOTS, one, 0)

    wait_faces(got[0], face_recv.at[0])

    def first_residual(s, carry):
        primal = []
        for f in range(NF):
            value = image[s, f] + picked(image, got[0], s, f)
            res[s, f] = value
            primal.append(column_sum(fold(weight[s, f] * scaled_of(s, f, value))))
        vec_buf[0, n, pl.ds(s * NF, NF), :] = jnp.concatenate(primal, axis=0)
        return carry

    lax.fori_loop(0, SLOTS, first_residual, 0)
    coarse_start(0)
    local_parts()
    lax.fori_loop(0, SLOTS, make_lift, 0)
    wait_rows(ITERS)
    wait_faces(over_deluxe, over_recv.at[0])
    wait_faces(over_inverse, over_recv.at[1])
    lax.fori_loop(0, SLOTS, over_tables, 0)
    coarse_middle(0)
    over_parts()
    wait_spread(top_buf, top_recv)
    coarse[...] = coarse_end(0)
    send_rows(0, coarse_row)
    norm_part = weigh()
    wait_rows(0)

    def first_direction(s, carry):
        for f in range(NF):
            value = weighted[s, f] + across_weighted(0, s, f)
            direc[s, f] = value
            half[s, pl.ds(f * FW, FW), :] = value.astype(BF16)
        return carry

    lax.fori_loop(0, SLOTS, first_direction, 0)
    wait_sent(got[0], face_send.at[0])
    curve_part = operate()
    reduce_start(0, norm_part, curve_part)
    send_all(image, 1)
    reduce_middle(0)
    wait_faces(got[1], face_recv.at[1])

    def full_image(s, carry):
        primal = []
        for f in range(NF):
            value = image[s, f] + picked(image, got[1], s, f)
            full[s, f] = value
            primal.append(column_sum(fold(lift[s, f] * value)))
        vec_buf[1, n, pl.ds(s * NF, NF), :] = jnp.concatenate(primal, axis=0)
        return carry

    lax.fori_loop(0, SLOTS, full_image, 0)
    coarse_start(1)
    norm, curve = reduce_end(0)
    step = norm / curve

    def next_residual(s, carry):
        for f in range(NF):
            value = res[s, f] - step * full[s, f]
            res[s, f] = value
            scaled_of(s, f, value)
        return carry

    lax.fori_loop(0, SLOTS, next_residual, 0)
    norm_part = local_parts()
    coarse_middle(1)
    second = (vec_buf[0, n] - step * vec_buf[1, n]) * (group[0] - step * group[1])
    norm_part = norm_part + (second[0:8] + second[8:16] + second[16:24])
    reduce_start(1, norm_part, norm_part)

    def next_solution(s, carry):
        for f in range(NF):
            sol[s, f] = sol[s, f] + step * direc[s, f]
        return carry

    lax.fori_loop(0, SLOTS, next_solution, 0)
    over_parts()
    coarse[...] = coarse[...] - step * coarse_end(1)
    send_rows(1, coarse_row)
    reduce_middle(1)
    weigh()
    entered = (every_buf[0] - step * every_buf[1]).reshape(wide * 8, FW)
    third_norm = column_sum(entered * (third[0] - step * third[1]))
    wait_rows(1)
    following, _ = reduce_end(1)
    following = following + third_norm
    ratio = following / norm

    def next_direction(s, carry):
        for f in range(NF):
            value = weighted[s, f] + across_weighted(1, s, f)
            value = value + ratio * direc[s, f]
            direc[s, f] = value
            half[s, pl.ds(f * FW, FW), :] = value.astype(BF16)
        return carry

    lax.fori_loop(0, SLOTS, next_direction, 0)
    wait_sent(got[1], face_send.at[1])
    curve_part = operate()
    reduce_start(2, curve_part, curve_part)
    send_all(image, 2)
    reduce_middle(2)
    wait_faces(got[2], face_recv.at[2])

    def last_image(s, carry):
        for f in range(NF):
            full[s, f] = image[s, f] + picked(image, got[2], s, f)
        return carry

    lax.fori_loop(0, SLOTS, last_image, 0)
    curve, _ = reduce_end(2)
    step_out[...] = following / curve
    wait_sent(got_half, half_send)
    wait_sent(got[2], face_send.at[2])
    wait_sent(over_deluxe, over_send.at[0])
    wait_sent(over_inverse, over_send.at[1])
    for i in range(ITERS + 1):
        wait_sent(rows_got[i], rows_send.at[i])
    for m in range(ITERS):
        wait_spread(part_buf.at[m], part_send.at[m])
        wait_spread(vec_buf.at[m], vec_send.at[m])
        wait_spread(every_buf.at[m], every_send.at[m])
    for k in range(REDUCES):
        wait_spread(plane_buf.at[k], plane_send.at[k])
        wait_spread(line_buf.at[k], line_send.at[k])
    wait_spread(top_buf, top_send)


def solution(mesh):
    wide, narrow = mesh.shape["wide"], mesh.shape["narrow"]
    faces = (SLOTS, NF, FW, FW)
    dma = pltpu.SemaphoreType.DMA

    def body(
        schur_matrix,
        face_inverse,
        deluxe,
        primal_weight,
        coarse_group,
        coarse_map,
        coarse_top,
        load_vector,
        previous,
        slot_count,
        partner,
        face_size,
    ):
        far = pl.BlockSpec(memory_space=pltpu.HBM)
        near = pl.BlockSpec(memory_space=pltpu.VMEM)
        scalar = pl.BlockSpec(memory_space=pltpu.SMEM)
        sol, direc, res, image, step = pl.pallas_call(
            functools.partial(kernel, wide, narrow),
            out_shape=[pltpu.VMEM(faces, F32)] * 4 + [pltpu.VMEM((1, FW), F32)],
            in_specs=[far, far, far, near, near, near, near, far, far, scalar, scalar, scalar],
            out_specs=[near] * 5,
            scratch_shapes=[
                pltpu.VMEM((SLOTS, NB, NB), BF16),
                pltpu.VMEM(faces, BF16),
                pltpu.VMEM(faces, BF16),
                pltpu.VMEM(faces, BF16),
                pltpu.VMEM(faces, BF16),
                pltpu.VMEM(faces, BF16),
                pltpu.VMEM(faces, F32),
                pltpu.VMEM(faces, F32),
                pltpu.VMEM(faces, F32),
                pltpu.VMEM(faces, F32),
                pltpu.VMEM(faces, F32),
                pltpu.VMEM((4, SLOTS, FW, FW), BF16),
                pltpu.VMEM((4, SLOTS, FW, FW), BF16),
                pltpu.VMEM((SLOTS, 4, FW, FW), BF16),
                pltpu.VMEM((SLOTS, 4, FW, FW), F32),
                pltpu.VMEM((SLOTS, 4, FW, FW), F32),
                pltpu.VMEM((SLOTS, NB, FW), BF16),
                pltpu.VMEM(faces, BF16),
                pltpu.VMEM((SLOTS * NF, FW), F32),
                pltpu.VMEM((ITERS, SLOTS * NF, FW), F32),
                pltpu.VMEM((ITERS, wide * 8, FW), F32),
                pltpu.VMEM((wide, 8, wide * 8), F32),
                pltpu.VMEM((4, SLOTS, FW, FW), BF16),
                *[pltpu.VMEM((4, SLOTS, FW, FW), F32)] * EXCHANGES,
                pltpu.VMEM((ITERS + 1, 4, 8, FW), F32),
                *[pltpu.VMEM((4, 8, FW), F32)] * (ITERS + 1),
                pltpu.VMEM((ITERS, narrow, SLOTS * NF, FW), F32),
                pltpu.VMEM((ITERS, narrow, 8, FW), F32),
                pltpu.VMEM((ITERS, wide, 8, FW), F32),
                pltpu.VMEM((REDUCES, wide, 2, FW), F32),
                pltpu.VMEM((REDUCES, narrow, 2, FW), F32),
                dma((5,)),
                dma((4,)),
                dma((4,)),
                dma((EXCHANGES, 4)),
                dma((EXCHANGES, 4)),
                dma((ITERS,)),
                dma((ITERS,)),
                dma((ITERS,)),
                dma((ITERS,)),
                dma((ITERS,)),
                dma((ITERS,)),
                dma((REDUCES,)),
                dma((REDUCES,)),
                dma((REDUCES,)),
                dma((REDUCES,)),
                dma(()),
                dma(()),
                dma((2, 4)),
                dma((2, 4)),
                dma((ITERS + 1, 4)),
                dma((ITERS + 1, 4)),
            ],
            compiler_params=pltpu.CompilerParams(
                collective_id=0, has_side_effects=True, vmem_limit_bytes=58880 * 1024
            ),
        )(
            schur_matrix[0, 0],
            face_inverse[0, 0],
            deluxe[0, 0],
            primal_weight[0, 0],
            coarse_group[0],
            coarse_map[0].T,
            coarse_top,
            load_vector[0, 0],
            previous[0, 0],
            slot_count,
            partner.reshape(SLOTS, 1, NF),
            face_size.reshape(SLOTS, 1, NF),
        )
        return (sol + step * direc)[None, None], (res - step * image)[None, None]

    both = ("wide", "narrow")
    deep = P(*both, None, None, None, None)
    return jax.shard_map(
        body,
        mesh=mesh,
        in_specs=(
            P(*both, None, None, None),
            deep,
            deep,
            P(*both, None, None, None),
            P(*both, None),
            P(*both, None),
            P("wide", None),
            deep,
            deep,
            P(*both),
            P(*both, None, None),
            P(*both, None, None),
        ),
        out_specs=(deep, deep),
        check_vma=False,
    )
```

```python
import functools

import jax
import jax.numpy as jnp
from jax import lax
from jax.experimental import pallas as pl
from jax.experimental.pallas import tpu as pltpu
from jax.sharding import PartitionSpec as P

ITERS = 2
SLOTS = 3
NF = 8
FW = 128
NB = NF * FW
MESH = pl.DeviceIdType.MESH
HIGH = lax.Precision.HIGHEST
F32 = jnp.float32
BF16 = jnp.bfloat16
EXCHANGES = ITERS + 1
REDUCES = 2 * ITERS - 1


def kernel(
    wide,
    narrow,
    schur_in,
    inverse_in,
    deluxe_in,
    weight_in,
    group_ref,
    map_ref,
    top_ref,
    load_in,
    previous_in,
    count_ref,
    partner_ref,
    size_ref,
    sol,
    direc,
    res,
    full,
    step_out,
    schur,
    inverse,
    deluxe,
    load,
    previous,
    turned,
    weight,
    image,
    weighted,
    local,
    lift,
    ahead,
    over_deluxe,
    over_inverse,
    over_turned,
    over_weight,
    over_local,
    half,
    scaled_half,
    coarse,
    group,
    third,
    top_buf,
    got_half,
    got_0,
    got_1,
    got_2,
    rows_out,
    rows_0,
    rows_1,
    rows_2,
    vec_buf,
    part_buf,
    every_buf,
    plane_buf,
    line_buf,
    load_sem,
    half_send,
    half_recv,
    face_send,
    face_recv,
    vec_send,
    vec_recv,
    part_send,
    part_recv,
    every_send,
    every_recv,
    plane_send,
    plane_recv,
    line_send,
    line_recv,
    top_send,
    top_recv,
    over_send,
    over_recv,
    rows_send,
    rows_recv,
):
    got = (got_0, got_1, got_2)
    rows_got = (rows_0, rows_1, rows_2)
    w = lax.axis_index("wide")
    n = lax.axis_index("narrow")

    loads = [
        pltpu.make_async_copy(previous_in, previous, load_sem.at[0]),
        pltpu.make_async_copy(deluxe_in, deluxe, load_sem.at[1]),
        pltpu.make_async_copy(schur_in, schur, load_sem.at[2]),
        pltpu.make_async_copy(load_in, load, load_sem.at[3]),
        pltpu.make_async_copy(inverse_in, inverse, load_sem.at[4]),
    ]
    for copy in loads:
        copy.start()

    barrier = pltpu.get_barrier_semaphore()

    def greet_wide(d, carry):
        pl.semaphore_signal(
            barrier, inc=1, device_id=(lax.rem(w + d, wide), n), device_id_type=MESH
        )
        return carry

    def greet_narrow(d, carry):
        pl.semaphore_signal(
            barrier, inc=1, device_id=(w, lax.rem(n + d, narrow)), device_id_type=MESH
        )
        return carry

    lax.fori_loop(1, wide, greet_wide, 0)
    lax.fori_loop(1, narrow, greet_narrow, 0)

    rows = lax.broadcasted_iota(jnp.int32, (FW, FW), 0)
    count = count_ref[0, 0]

    def inside(s, f):
        size = jnp.where(s < count, size_ref[s, 0, f], 0)
        return rows < size

    def masked(s, f, values):
        return jnp.where(inside(s, f), values, 0.0)

    def picked(values, arrived, s, f):
        t = partner_ref[s, 0, f]
        slot = jnp.maximum(t, 0)
        source = arrived[f, slot] if f < 4 else values[slot, f ^ 1]
        return jnp.where(t >= 0, source.astype(F32), 0.0)

    above = (w, lax.rem(n + 1, narrow))
    below = (w, lax.rem(n + narrow - 1, narrow))
    right = (lax.rem(w + 1, wide), n)
    left = (lax.rem(w + wide - 1, wide), n)

    def send_face(values, arrived, send, recv, s, f, to, device):
        pltpu.make_async_remote_copy(
            src_ref=values.at[s, f],
            dst_ref=arrived.at[to, s],
            send_sem=send.at[to],
            recv_sem=recv.at[to],
            device_id=device,
            device_id_type=MESH,
        ).start()

    def send_narrow(values, arrived, send, recv, s):
        @pl.when(n < narrow - 1)
        def _():
            send_face(values, arrived, send, recv, s, 1, 0, above)

        @pl.when(n > 0)
        def _():
            send_face(values, arrived, send, recv, s, 0, 1, below)

    def send_wide(values, arrived, send, recv, s):
        send_face(values, arrived, send, recv, s, 3, 2, right)
        send_face(values, arrived, send, recv, s, 2, 3, left)

    def send_faces(values, arrived, send, recv, s):
        send_narrow(values, arrived, send, recv, s)
        send_wide(values, arrived, send, recv, s)

    def send_rows(i, row_of):
        for to, f in ((0, 1), (1, 0), (2, 3), (3, 2)):
            rows_out[i, to] = jnp.concatenate(
                [row_of(s, f) for s in range(SLOTS)] + [jnp.zeros((8 - SLOTS, FW), F32)], axis=0
            )
        to_above, to_below, to_right, to_left = [
            pltpu.make_async_remote_copy(
                src_ref=rows_out.at[i, to],
                dst_ref=rows_got[i].at[to],
                send_sem=rows_send.at[i, to],
                recv_sem=rows_recv.at[i, to],
                device_id=device,
                device_id_type=MESH,
            )
            for to, device in enumerate((above, below, right, left))
        ]

        @pl.when(n < narrow - 1)
        def _():
            to_above.start()

        @pl.when(n > 0)
        def _():
            to_below.start()

        to_right.start()
        to_left.start()

    def wait_bytes(ref, sem):
        pltpu.make_async_copy(ref, ref, sem).wait()

    def wait_faces(arrived, recv):
        @pl.when(n > 0)
        def _():
            wait_bytes(arrived.at[0], recv.at[0])

        @pl.when(n < narrow - 1)
        def _():
            wait_bytes(arrived.at[1], recv.at[1])

        wait_bytes(arrived.at[2], recv.at[2])
        wait_bytes(arrived.at[3], recv.at[3])

    def wait_sent(arrived, send):
        @pl.when(n < narrow - 1)
        def _():
            wait_bytes(arrived.at[0], send.at[0])

        @pl.when(n > 0)
        def _():
            wait_bytes(arrived.at[1], send.at[1])

        wait_bytes(arrived.at[2], send.at[2])
        wait_bytes(arrived.at[3], send.at[3])

    def spread_narrow(buf, send, recv):
        def one(d, carry):
            pltpu.make_async_remote_copy(
                src_ref=buf.at[n],
                dst_ref=buf.at[n],
                send_sem=send,
                recv_sem=recv,
                device_id=(w, lax.rem(n + d, narrow)),
                device_id_type=MESH,
            ).start()
            return carry

        lax.fori_loop(1, narrow, one, 0)

    def spread_wide(buf, send, recv):
        def one(d):
            pltpu.make_async_remote_copy(
                src_ref=buf.at[w],
                dst_ref=buf.at[w],
                send_sem=send,
                recv_sem=recv,
                device_id=(lax.rem(w + d, wide), n),
                device_id_type=MESH,
            ).start()

        def four(i, carry):
            for d in range(4):
                one(4 * i + d)
            return carry

        for d in range(1, 4):
            one(d)
        lax.fori_loop(1, wide // 4, four, 0)

    def wait_spread(buf, sem):
        wait_bytes(buf.at[pl.ds(0, buf.shape[0] - 1)], sem)

    def fold(product):
        return jnp.sum(product.reshape(FW // 8, 8, FW), axis=0)

    def reduce_start(k, first, second):
        plane_buf[k, w] = jnp.concatenate(
            [jnp.sum(first, axis=0, keepdims=True), jnp.sum(second, axis=0, keepdims=True)], axis=0
        )
        spread_wide(plane_buf.at[k], plane_send.at[k], plane_recv.at[k])

    def reduce_middle(k):
        wait_spread(plane_buf.at[k], plane_recv.at[k])
        line_buf[k, n] = jnp.sum(plane_buf[k], axis=0)
        spread_narrow(line_buf.at[k], line_send.at[k], line_recv.at[k])

    def reduce_end(k):
        wait_spread(line_buf.at[k], line_recv.at[k])
        total = jnp.sum(line_buf[k], axis=0)
        return total[0:1], total[1:2]

    def spread_weight(s, carry):
        for f in range(NF):
            row = weight_in[s, f : f + 1, :]
            column = jnp.broadcast_to(row, (FW, FW)).T
            weight[s, f] = masked(s, f, column)
        return carry

    lax.fori_loop(0, SLOTS, spread_weight, 0)
    loads[1].wait()

    def turn(s, carry):
        for f in range(NF):
            turned[s, f] = deluxe[s, f].T
        return carry

    lax.fori_loop(0, SLOTS, turn, 0)
    loads[0].wait()
    pl.semaphore_wait(barrier, wide + narrow - 2)

    for s in range(SLOTS):
        send_faces(previous, got_half, half_send, half_recv, s)
    send_rows(ITERS, lambda s, f: weight_in[s, f : f + 1, :])
    for s in range(SLOTS):
        send_faces(deluxe, over_deluxe, over_send.at[0], over_recv.at[0], s)
    loads[4].wait()
    for s in range(SLOTS):
        send_faces(inverse, over_inverse, over_send.at[1], over_recv.at[1], s)
    top_buf[w] = top_ref[...]
    spread_wide(top_buf, top_send, top_recv)

    def average(faces):
        def one(s, carry):
            for f in faces:
                own = previous[s, f].astype(F32)
                across = picked(previous, got_half, s, f)
                mean = jnp.where(partner_ref[s, 0, f] >= 0, 0.5 * (own + across), own)
                mean = masked(s, f, mean)
                sol[s, f] = mean
                half[s, pl.ds(f * FW, FW), :] = mean.astype(BF16)
            return carry

        lax.fori_loop(0, SLOTS, one, 0)

    def go_ahead(s, carry):
        ahead[s] = jnp.dot(
            schur[s, :, NB // 2 :], half[s, pl.ds(NB // 2, NB // 2), :], preferred_element_type=F32
        )
        return carry

    def rest_of_product(s):
        return ahead[s] + jnp.dot(
            schur[s, :, : NB // 2], half[s, pl.ds(0, NB // 2), :], preferred_element_type=F32
        )

    average(range(4, NF))
    loads[2].wait()
    lax.fori_loop(0, SLOTS, go_ahead, 0)
    wait_faces(got_half, half_recv)
    average(range(4))
    loads[3].wait()

    def start_residual(s, carry):
        product = rest_of_product(s)
        for f in range(NF):
            image[s, f] = masked(
                s, f, load[s, f].astype(F32) - product[f * FW : (f + 1) * FW]
            )
        send_faces(image, got[0], face_send.at[0], face_recv.at[0], s)
        return carry

    lax.fori_loop(0, SLOTS, start_residual, 0)
    zero = jnp.zeros((8, FW), F32)

    def scaled_of(s, f, values):
        scaled = masked(
            s, f, jnp.dot(turned[s, f], values.astype(BF16), preferred_element_type=F32)
        )
        scaled_half[s, f] = scaled.astype(BF16)
        return scaled

    def column_sum(values):
        return jnp.sum(values, axis=0, keepdims=True)

    def coarse_start(m):
        entering = vec_buf[m, n]
        part_buf[m, n] = jnp.dot(map_ref[...], entering, precision=HIGH)
        spread_narrow(part_buf.at[m], part_send.at[m], part_recv.at[m])
        spread_narrow(vec_buf.at[m], vec_send.at[m], vec_recv.at[m])

    def local_parts():
        def one(s, total):
            for f in range(NF):
                entering = scaled_half[s, f]
                value = masked(
                    s, f, jnp.dot(inverse[s, f], entering, preferred_element_type=F32)
                )
                local[s, f] = value
                total = total + fold(entering.astype(F32) * value)
            return total

        return lax.fori_loop(0, SLOTS, one, zero)

    def over_tables(s, carry):
        for f in range(4):
            slot = jnp.maximum(partner_ref[s, 0, f], 0)
            over_turned[s, f] = over_deluxe[f, slot].T
            row = rows_2[f, pl.ds(slot, 1), :]
            over_weight[s, f] = masked(s, f, jnp.broadcast_to(row, (FW, FW)).T)
        return carry

    def over_parts():
        def one(s, carry):
            for f in range(4):
                slot = jnp.maximum(partner_ref[s, 0, f], 0)
                scaled = masked(
                    s,
                    f,
                    jnp.dot(
                        over_turned[s, f], res[s, f].astype(BF16), preferred_element_type=F32
                    ),
                )
                over_local[s, f] = masked(
                    s,
                    f,
                    jnp.dot(
                        over_inverse[f, slot], scaled.astype(BF16), preferred_element_type=F32
                    ),
                )
            return carry

        lax.fori_loop(0, SLOTS, one, 0)

    def across_weighted(m, s, f):
        t = partner_ref[s, 0, f]
        slot = jnp.maximum(t, 0)
        if f < 4:
            out = rows_got[m][f, pl.ds(slot, 1), :]
            correction = (over_local[s, f] + over_weight[s, f] * out).astype(BF16)
            value = masked(
                s, f, jnp.dot(over_deluxe[f, slot], correction, preferred_element_type=F32)
            )
        else:
            value = weighted[slot, f ^ 1]
        return jnp.where(t >= 0, value, 0.0)

    def coarse_row(s, f):
        return coarse[s * NF + f : s * NF + f + 1, :]

    def wait_rows(i):
        wait_faces(rows_got[i], rows_recv.at[i])

    def make_lift(s, carry):
        for f in range(NF):
            value = weight[s, f]
            main = value.astype(BF16)
            rest = (value - main.astype(F32)).astype(BF16)
            lift[s, f] = jnp.dot(deluxe[s, f], main, preferred_element_type=F32) + jnp.dot(
                deluxe[s, f], rest, preferred_element_type=F32
            )
        return carry

    def coarse_middle(m):
        wait_spread(part_buf.at[m], part_recv.at[m])
        every_buf[m, w] = jnp.sum(part_buf[m], axis=0)
        spread_wide(every_buf.at[m], every_send.at[m], every_recv.at[m])
        wait_spread(vec_buf.at[m], vec_recv.at[m])
        group[m] = jnp.dot(
            group_ref[...], vec_buf[m].reshape(narrow * SLOTS * NF, FW), precision=HIGH
        )

    def coarse_end(m):
        wait_spread(every_buf.at[m], every_recv.at[m])
        third[m] = jnp.dot(
            top_buf[...].reshape(wide * 8, wide * 8),
            every_buf[m].reshape(wide * 8, FW),
            precision=HIGH,
        )
        own = third[m, pl.ds(pl.multiple_of(w * 8, 8), 8), :]
        return group[m] + lax.dot_general(
            map_ref[...], own, (((0,), (0,)), ((), ())), precision=HIGH
        )

    def weigh():
        def one(s, total):
            for f in range(NF):
                out = coarse[pl.ds(s * NF + f, 1), :]
                correction = (local[s, f] + weight[s, f] * out).astype(BF16)
                value = masked(
                    s, f, jnp.dot(deluxe[s, f], correction, preferred_element_type=F32)
                )
                weighted[s, f] = value
                total = total + fold(res[s, f] * value)
            return total

        return lax.fori_loop(0, SLOTS, one, zero)

    def operate(e, begun):
        def one(s, total):
            if begun:
                product = rest_of_product(s)
            else:
                product = jnp.dot(schur[s], half[s], preferred_element_type=F32)
            for f in range(NF):
                value = masked(s, f, product[f * FW : (f + 1) * FW])
                image[s, f] = value
                total = total + fold(direc[s, f] * value)
            send_narrow(image, got[e], face_send.at[e], face_recv.at[e], s)
            return total

        return lax.fori_loop(0, SLOTS, one, zero)

    def send_sideways(e):
        def one(s, carry):
            send_wide(image, got[e], face_send.at[e], face_recv.at[e], s)
            return carry

        lax.fori_loop(0, SLOTS, one, 0)

    wait_faces(got[0], face_recv.at[0])

    def first_residual(s, carry):
        primal = []
        for f in range(NF):
            value = image[s, f] + picked(image, got[0], s, f)
            res[s, f] = value
            primal.append(column_sum(fold(weight[s, f] * scaled_of(s, f, value))))
        vec_buf[0, n, pl.ds(s * NF, NF), :] = jnp.concatenate(primal, axis=0)
        return carry

    lax.fori_loop(0, SLOTS, first_residual, 0)
    coarse_start(0)
    local_parts()
    lax.fori_loop(0, SLOTS, make_lift, 0)
    wait_rows(ITERS)
    wait_faces(over_deluxe, over_recv.at[0])
    wait_faces(over_inverse, over_recv.at[1])
    lax.fori_loop(0, SLOTS, over_tables, 0)
    coarse_middle(0)
    over_parts()
    wait_spread(top_buf, top_recv)
    coarse[...] = coarse_end(0)
    send_rows(0, coarse_row)
    norm_part = weigh()

    def first_direction(faces):
        def one(s, carry):
            for f in faces:
                value = weighted[s, f] + across_weighted(0, s, f)
                direc[s, f] = value
                half[s, pl.ds(f * FW, FW), :] = value.astype(BF16)
            return carry

        lax.fori_loop(0, SLOTS, one, 0)

    first_direction(range(4, NF))
    lax.fori_loop(0, SLOTS, go_ahead, 0)
    wait_rows(0)
    first_direction(range(4))
    wait_sent(got[0], face_send.at[0])
    curve_part = operate(1, True)
    reduce_start(0, norm_part, curve_part)
    send_sideways(1)
    reduce_middle(0)
    wait_faces(got[1], face_recv.at[1])

    def full_image(s, carry):
        primal = []
        for f in range(NF):
            value = image[s, f] + picked(image, got[1], s, f)
            full[s, f] = value
            primal.append(column_sum(fold(lift[s, f] * value)))
        vec_buf[1, n, pl.ds(s * NF, NF), :] = jnp.concatenate(primal, axis=0)
        return carry

    lax.fori_loop(0, SLOTS, full_image, 0)
    coarse_start(1)
    norm, curve = reduce_end(0)
    step = norm / curve

    def next_residual(s, carry):
        for f in range(NF):
            value = res[s, f] - step * full[s, f]
            res[s, f] = value
            scaled_of(s, f, value)
        return carry

    lax.fori_loop(0, SLOTS, next_residual, 0)
    norm_part = local_parts()
    coarse_middle(1)
    second = (vec_buf[0, n] - step * vec_buf[1, n]) * (group[0] - step * group[1])
    norm_part = norm_part + (second[0:8] + second[8:16] + second[16:24])
    reduce_start(1, norm_part, norm_part)

    def next_solution(s, carry):
        for f in range(NF):
            sol[s, f] = sol[s, f] + step * direc[s, f]
        return carry

    lax.fori_loop(0, SLOTS, next_solution, 0)
    over_parts()
    coarse[...] = coarse[...] - step * coarse_end(1)
    send_rows(1, coarse_row)
    reduce_middle(1)
    weigh()
    entered = (every_buf[0] - step * every_buf[1]).reshape(wide * 8, FW)
    third_norm = column_sum(entered * (third[0] - step * third[1]))
    wait_rows(1)
    following, _ = reduce_end(1)
    following = following + third_norm
    ratio = following / norm

    def next_direction(s, carry):
        for f in range(NF):
            value = weighted[s, f] + across_weighted(1, s, f)
            value = value + ratio * direc[s, f]
            direc[s, f] = value
            half[s, pl.ds(f * FW, FW), :] = value.astype(BF16)
        return carry

    lax.fori_loop(0, SLOTS, next_direction, 0)
    wait_sent(got[1], face_send.at[1])
    curve_part = operate(2, False)
    reduce_start(2, curve_part, curve_part)
    send_sideways(2)
    reduce_middle(2)
    wait_faces(got[2], face_recv.at[2])

    def last_image(s, carry):
        for f in range(NF):
            full[s, f] = image[s, f] + picked(image, got[2], s, f)
        return carry

    lax.fori_loop(0, SLOTS, last_image, 0)
    curve, _ = reduce_end(2)
    step_out[...] = following / curve
    wait_sent(got_half, half_send)
    wait_sent(got[2], face_send.at[2])
    wait_sent(over_deluxe, over_send.at[0])
    wait_sent(over_inverse, over_send.at[1])
    for i in range(ITERS + 1):
        wait_sent(rows_got[i], rows_send.at[i])
    for m in range(ITERS):
        wait_spread(part_buf.at[m], part_send.at[m])
        wait_spread(vec_buf.at[m], vec_send.at[m])
        wait_spread(every_buf.at[m], every_send.at[m])
    for k in range(REDUCES):
        wait_spread(plane_buf.at[k], plane_send.at[k])
        wait_spread(line_buf.at[k], line_send.at[k])
    wait_spread(top_buf, top_send)


def solution(mesh):
    wide, narrow = mesh.shape["wide"], mesh.shape["narrow"]
    faces = (SLOTS, NF, FW, FW)
    dma = pltpu.SemaphoreType.DMA

    def body(
        schur_matrix,
        face_inverse,
        deluxe,
        primal_weight,
        coarse_group,
        coarse_map,
        coarse_top,
        load_vector,
        previous,
        slot_count,
        partner,
        face_size,
    ):
        far = pl.BlockSpec(memory_space=pltpu.HBM)
        near = pl.BlockSpec(memory_space=pltpu.VMEM)
        scalar = pl.BlockSpec(memory_space=pltpu.SMEM)
        sol, direc, res, image, step = pl.pallas_call(
            functools.partial(kernel, wide, narrow),
            out_shape=[pltpu.VMEM(faces, F32)] * 4 + [pltpu.VMEM((1, FW), F32)],
            in_specs=[far, far, far, near, near, near, near, far, far, near, scalar, scalar],
            out_specs=[near] * 5,
            scratch_shapes=[
                pltpu.VMEM((SLOTS, NB, NB), BF16),
                pltpu.VMEM(faces, BF16),
                pltpu.VMEM(faces, BF16),
                pltpu.VMEM(faces, BF16),
                pltpu.VMEM(faces, BF16),
                pltpu.VMEM(faces, BF16),
                pltpu.VMEM(faces, F32),
                pltpu.VMEM(faces, F32),
                pltpu.VMEM(faces, F32),
                pltpu.VMEM(faces, F32),
                pltpu.VMEM(faces, F32),
                pltpu.VMEM((SLOTS, NB, FW), F32),
                pltpu.VMEM((4, SLOTS, FW, FW), BF16),
                pltpu.VMEM((4, SLOTS, FW, FW), BF16),
                pltpu.VMEM((SLOTS, 4, FW, FW), BF16),
                pltpu.VMEM((SLOTS, 4, FW, FW), F32),
                pltpu.VMEM((SLOTS, 4, FW, FW), F32),
                pltpu.VMEM((SLOTS, NB, FW), BF16),
                pltpu.VMEM(faces, BF16),
                pltpu.VMEM((SLOTS * NF, FW), F32),
                pltpu.VMEM((ITERS, SLOTS * NF, FW), F32),
                pltpu.VMEM((ITERS, wide * 8, FW), F32),
                pltpu.VMEM((wide, 8, wide * 8), F32),
                pltpu.VMEM((4, SLOTS, FW, FW), BF16),
                *[pltpu.VMEM((4, SLOTS, FW, FW), F32)] * EXCHANGES,
                pltpu.VMEM((ITERS + 1, 4, 8, FW), F32),
                *[pltpu.VMEM((4, 8, FW), F32)] * (ITERS + 1),
                pltpu.VMEM((ITERS, narrow, SLOTS * NF, FW), F32),
                pltpu.VMEM((ITERS, narrow, 8, FW), F32),
                pltpu.VMEM((ITERS, wide, 8, FW), F32),
                pltpu.VMEM((REDUCES, wide, 2, FW), F32),
                pltpu.VMEM((REDUCES, narrow, 2, FW), F32),
                dma((5,)),
                dma((4,)),
                dma((4,)),
                dma((EXCHANGES, 4)),
                dma((EXCHANGES, 4)),
                dma((ITERS,)),
                dma((ITERS,)),
                dma((ITERS,)),
                dma((ITERS,)),
                dma((ITERS,)),
                dma((ITERS,)),
                dma((REDUCES,)),
                dma((REDUCES,)),
                dma((REDUCES,)),
                dma((REDUCES,)),
                dma(()),
                dma(()),
                dma((2, 4)),
                dma((2, 4)),
                dma((ITERS + 1, 4)),
                dma((ITERS + 1, 4)),
            ],
            compiler_params=pltpu.CompilerParams(
                collective_id=0, has_side_effects=True, vmem_limit_bytes=58880 * 1024
            ),
        )(
            schur_matrix[0, 0],
            face_inverse[0, 0],
            deluxe[0, 0],
            primal_weight[0, 0],
            coarse_group[0],
            coarse_map[0].T,
            coarse_top,
            load_vector[0, 0],
            previous[0, 0],
            slot_count,
            partner.reshape(SLOTS, 1, NF),
            face_size.reshape(SLOTS, 1, NF),
        )
        return (sol + step * direc)[None, None], (res - step * image)[None, None]

    both = ("wide", "narrow")
    deep = P(*both, None, None, None, None)
    return jax.shard_map(
        body,
        mesh=mesh,
        in_specs=(
            P(*both, None, None, None),
            deep,
            deep,
            P(*both, None, None, None),
            P(*both, None),
            P(*both, None),
            P("wide", None),
            deep,
            deep,
            P(*both),
            P(*both, None, None),
            P(*both, None, None),
        ),
        out_specs=(deep, deep),
        check_vma=False,
    )
```
